32 devices in a mesh: node: 8 (over z, y), local: 4 (over x, core).
Axes of the slice: x: 2, y: 2, z: 4, core: 2. Of those that a mesh axis runs over, the one named last changes fastest.
Arguments:
- tokens: bfloat16 [4096, 2048], P(('node', 'local')), may hold values from -6 to 6
- norm_gain: float32 [2048], replicated, may hold values from 0.1 to 1.9
- router_weight: bfloat16 [2048, 16], replicated, may hold values from -0.125 to 0.125
- placement: int32 [16], replicated, may hold values from 0 to 15, each once
- expert_ids: int32 [4096, 6], P(('node', 'local')), may hold values from 0 to 15, all different within a row; in each aligned block of 128 rows (0 to 127, 128 to 255, ...) at most 72 rows name the same one
- w_gate: bfloat16 [2048, 22528], P(None, ('node', 'local')), may hold values from -0.125 to 0.125
- w_up: bfloat16 [2048, 22528], P(None, ('node', 'local')), may hold values from -0.125 to 0.125
- w_down: bfloat16 [22528, 2048], P(('node', 'local')), may hold values from -0.15625 to 0.15625
- shared_gate: bfloat16 [2048, 2816], P(None, 'local'), may hold values from -0.125 to 0.125
- shared_up: bfloat16 [2048, 2816], P(None, 'local'), may hold values from -0.125 to 0.125
- shared_down: bfloat16 [2816, 2048], P('local'), may hold values from -0.109375 to 0.109375
Outputs:
- moe_out: bfloat16 [4096, 2048], P(('node', 'local'))
The draws below stay inside these ranges and needn't reach their ends.
Inputs may be any that keep to these rules, and one draw needn't show every extreme that they name: Expert e's weights stand in slot placement[e]; every slot holds one expert. `expert_ids`: each row names 6 different experts. Among the rows of one device (aligned blocks of 128 rows) no expert is named more than 72 times, a bound that some block reaches.
All inputs are finite; a program needn't handle non-finite values.
Results may differ from the reference program's by a relative error of at most 0.011.
Values may be sent and summed in bfloat16 or wider, within the bound.
A program may use at most 128 MiB of HBM per device.

```python
import math
import jax
import jax.numpy as jnp
import numpy as np
from jax import lax

D = 2048
FE = 1408
FS = 2816
TOPK = 6
TOK_DEV = 128
EXPERTS = 16
HALF = 704
CAP = 72
TOKENS = 4096
DEVICES = 32


def levels(key, dims, shards, smallest, high):
    def one(dim, shards_of):
        draws = jax.random.uniform(jax.random.fold_in(jax.random.fold_in(key, 6), dim), (shards_of,), jnp.float32, smallest / len(shards), high / len(shards))
        return jnp.repeat(jnp.exp(draws), dims[dim] // shards_of).reshape((-1,) + (1,) * (len(dims) - dim - 1))

    gain = one(*shards[0])
    for cut in shards[1:]:
        gain = gain * one(*cut)
    return gain


def routed_block(rng, own, number, rows, number_of, top, most, slope):
    order = jax.random.permutation(rng, number_of)
    packed, usual = portions_of(number_of, rows * top, most, slope, True), portions_of(number_of, rows * top, most, slope, False)
    places = jnp.arange(number_of)

    def named(tallies, turn):
        used = int((tallies > 0).sum())
        fixed = max(1, used // 4)
        moved = fixed + (places - fixed + turn * (used - fixed)) % max(1, number_of - fixed)
        return jnp.zeros((number_of,), jnp.int32).at[order[jnp.where(places < fixed, places, moved)]].set(jnp.asarray(tallies, jnp.int32))

    tallies = jnp.where(number % 4 == 0, named(packed, number // 4), named(usual, number - number // 4 - 1))
    mixed = jax.random.permutation(jax.random.fold_in(own, 3), number_of)
    giver, receiver = mixed[0:number_of // 2 * 2:2], mixed[1:number_of // 2 * 2:2]
    room = jnp.minimum(tallies[giver] - 1, most - tallies[receiver]) // 2
    room = jnp.where((giver == order[0]) | (receiver == order[0]) | (tallies[receiver] == 0), 0, jnp.maximum(room, 0))
    moved = jax.random.randint(jax.random.fold_in(own, 4), (number_of // 2,), 0, 1 << 20) % (room + 1)
    tallies = tallies.at[giver].add(-moved).at[receiver].add(moved)
    items = jnp.searchsorted(jnp.cumsum(tallies), jnp.arange(rows * top), side="right").astype(jnp.int32)
    grid = items.reshape(top, rows).T
    grid = grid[jax.random.permutation(jax.random.fold_in(own, 1), rows)]
    turn = jax.random.randint(jax.random.fold_in(own, 2), (rows, 1), 0, top)
    return jnp.take_along_axis(grid, (jnp.arange(top)[None, :] + turn) % top, axis=1)


def portions_of(number_of, total, reach, lean, full):
    portions = [(1 << 20) // math.isqrt(rank ** lean) + 1 for rank in range(1, number_of + 1)]
    largest = reach if full else min(reach, max(-(-total // number_of), total * portions[0] // sum(portions)))
    least = 1 if total - largest >= number_of - 1 else 0
    counts, surplus = [largest] + [least] * (number_of - 1), total - largest - least * (number_of - 1)
    while surplus > 0:
        candidates = [i for i in range(1, number_of) if counts[i] < largest] or [i for i in range(1, number_of) if counts[i] < reach]
        whole, left = sum([portions[i] for i in candidates]), surplus
        for i in candidates:
            addition = min(reach - counts[i], max(1, left * portions[i] // whole), surplus)
            counts[i] = counts[i] + addition
            surplus = surplus - addition
    return np.array(counts)


def centred(stream_key, shape, width, most, cuts=(), held_as=jnp.bfloat16):
    factor_of = levels(stream_key, shape, cuts, -0.22, 0.18) if cuts else 1.0
    array = jax.random.normal(stream_key, shape, jnp.float32) * width * factor_of
    return jnp.minimum(jnp.maximum(array, -most), most).astype(held_as)


def setup_inputs(seed: int = 0) -> dict:
    streams_of = jax.random.split(jax.random.key(seed), 12)
    tokens = centred(streams_of[0], (TOKENS, D), 1.0, 6.0, ((0, 32),))
    norm_gain = jnp.clip(1.0 + 0.18 * jax.random.normal(streams_of[1], (D,), jnp.float32), 0.1, 1.9)
    router_weight = centred(streams_of[2], (D, EXPERTS), D ** -0.5, 0.125)
    placement = jax.random.permutation(streams_of[3], EXPERTS).astype(jnp.int32)
    expert_ids_keys = jax.random.split(jax.random.fold_in(streams_of[4], 1), TOKENS // TOK_DEV)
    expert_ids_turns = jax.random.permutation(jax.random.fold_in(streams_of[4], 3), TOKENS // TOK_DEV)
    expert_ids = jax.vmap(lambda own, number: routed_block(jax.random.fold_in(streams_of[4], 2), own, number, TOK_DEV, EXPERTS, TOPK, CAP, 2))(expert_ids_keys, expert_ids_turns).reshape((TOKENS, TOPK))
    w_gate = centred(streams_of[5], (D, EXPERTS * FE), D ** -0.5, 0.125, ((1, 32),))
    w_up = centred(streams_of[6], (D, EXPERTS * FE), D ** -0.5, 0.125, ((1, 32),))
    w_down = centred(streams_of[7], (EXPERTS * FE, D), FE ** -0.5, 0.15625, ((0, 32),))
    shared_gate = centred(streams_of[8], (D, FS), D ** -0.5, 0.125, ((1, 4),))
    shared_up = centred(streams_of[9], (D, FS), D ** -0.5, 0.125, ((1, 4),))
    shared_down = centred(streams_of[10], (FS, D), FS ** -0.5, 0.109375, ((0, 4),))
    return dict(tokens=tokens, norm_gain=norm_gain, router_weight=router_weight, placement=placement, expert_ids=expert_ids, w_gate=w_gate, w_up=w_up, w_down=w_down, shared_gate=shared_gate, shared_up=shared_up, shared_down=shared_down)


def feed_forward(row_block, gate_cols, up_cols, down_rows):
    gate_proj = jnp.dot(row_block, gate_cols, preferred_element_type=jnp.float32)
    up_proj = jnp.dot(row_block, up_cols, preferred_element_type=jnp.float32)
    activated = (jax.nn.silu(gate_proj) * up_proj).astype(jnp.bfloat16)
    return jnp.dot(activated, down_rows, preferred_element_type=jnp.float32)

def reference(tokens, norm_gain, router_weight, placement, expert_ids, w_gate, w_up, w_down, shared_gate, shared_up, shared_down):
    floats = tokens.astype(jnp.float32)
    normed = (floats * lax.rsqrt(lax.optimization_barrier(jnp.mean(floats * floats, -1, keepdims=True)) + 1e-06) * norm_gain).astype(jnp.bfloat16)
    logits = jnp.dot(normed, router_weight, preferred_element_type=jnp.float32)
    scores = jax.nn.sigmoid(logits)
    picked = jnp.take_along_axis(scores, expert_ids, 1)
    gate_weights = (picked / lax.optimization_barrier(jnp.sum(picked, -1, keepdims=True))).astype(jnp.bfloat16)
    slots = placement[expert_ids].astype(jnp.int32)
    expert_iota = jnp.arange(EXPERTS, dtype=jnp.int32)
    slot_hot = (slots[:, :, None] == expert_iota).astype(jnp.int32).reshape(DEVICES, TOK_DEV * TOPK, EXPERTS)
    position = lax.optimization_barrier(jnp.sum((jnp.cumsum(slot_hot, 1) - 1) * slot_hot, -1)).astype(jnp.int32)
    source = jnp.broadcast_to(jnp.arange(DEVICES, dtype=jnp.int32)[:, None], (DEVICES, TOK_DEV * TOPK))
    flat_slot = slots.reshape(DEVICES, TOK_DEV * TOPK)
    index = ((flat_slot * DEVICES + source) * CAP + position).reshape(-1).astype(jnp.int32)
    token_index = jnp.repeat(jnp.arange(TOKENS, dtype=jnp.int32), TOPK)
    table = jnp.full((EXPERTS * DEVICES * CAP,), TOKENS, jnp.int32).at[index].set(token_index)
    weight_table = jnp.zeros((EXPERTS * DEVICES * CAP,), jnp.float32).at[index].set(gate_weights.reshape(-1).astype(jnp.float32))
    padded = jnp.concatenate([normed, jnp.zeros((1, D), jnp.bfloat16)], 0)

    def one_slot(running_sum, slot_index):
        begin = (slot_index * DEVICES * CAP).astype(jnp.int32)
        rows_index = lax.dynamic_slice_in_dim(table, begin, DEVICES * CAP)
        row_weights = lax.dynamic_slice_in_dim(weight_table, begin, DEVICES * CAP)
        row_block = padded[rows_index]
        gate_cols = lax.dynamic_slice_in_dim(w_gate, (slot_index * FE).astype(jnp.int32), FE, 1)
        up_cols = lax.dynamic_slice_in_dim(w_up, (slot_index * FE).astype(jnp.int32), FE, 1)
        down_rows = lax.dynamic_slice_in_dim(w_down, (slot_index * FE).astype(jnp.int32), FE, 0)
        total = jnp.zeros((DEVICES * CAP, D), jnp.float32)
        for half_index in range(2):
            lower = half_index * HALF
            partial_value = feed_forward(row_block, gate_cols[:, lower:lower + HALF], up_cols[:, lower:lower + HALF], down_rows[lower:lower + HALF]).astype(jnp.bfloat16)
            total = total + partial_value.astype(jnp.float32)
        expert_out = total.astype(jnp.bfloat16)
        running_sum = running_sum.at[rows_index].add(row_weights[:, None] * expert_out.astype(jnp.float32), mode='drop')
        return (running_sum, None)
    routed, _ = lax.scan(one_slot, jnp.zeros((TOKENS, D), jnp.float32), jnp.arange(EXPERTS, dtype=jnp.int32))
    shared = feed_forward(normed, shared_gate, shared_up, shared_down)
    return (shared + routed).astype(jnp.bfloat16)
```

```python
import jax
import jax.numpy as jnp
from jax import lax
from jax.experimental import pallas as pl
from jax.experimental.pallas import tpu as pltpu
from jax.sharding import PartitionSpec as P


def partner_2(block, axis, bit):
    count = lax.axis_size(axis)
    route = []
    for low in range(count):
        high = low | 1 << bit
        if high != low and high < count:
            route += [(low, high), (high, low)]
    return lax.ppermute(block, axis, route)


def feed_forward(row_block, gate_cols, up_cols, down_rows):
    gate_proj = jnp.dot(row_block, gate_cols, preferred_element_type=jnp.float32)
    up_proj = jnp.dot(row_block, up_cols, preferred_element_type=jnp.float32)
    activated = (jax.nn.silu(gate_proj) * up_proj).astype(jnp.bfloat16)
    return jnp.dot(activated, down_rows, preferred_element_type=jnp.float32)


def body(
    tokens,
    norm_gain,
    router_weight,
    placement,
    expert_ids,
    w_gate,
    w_up,
    w_down,
    shared_gate,
    shared_up,
    shared_down,
):
    floats = tokens.astype(jnp.float32)
    normed = (
        floats * lax.rsqrt(jnp.mean(floats * floats, -1, keepdims=True) + 1e-06) * norm_gain
    ).astype(jnp.bfloat16)
    tok_rows = normed.shape[0]
    model_width = normed.shape[1]
    gathered = lax.all_gather(normed, "local", axis=0, tiled=True)
    shared = lax.psum_scatter(
        feed_forward(gathered, shared_gate, shared_up, shared_down),
        "local",
        scatter_dimension=0,
        tiled=True,
    )
    top_count = expert_ids.shape[1]
    experts = placement.shape[0]
    capacity = 3 * tok_rows * top_count // (2 * experts)
    logits = jnp.dot(normed, router_weight, preferred_element_type=jnp.float32)
    scores = jax.nn.sigmoid(logits)
    expert_iota = jnp.arange(experts, dtype=jnp.int32)
    id_hot = expert_ids[:, :, None] == expert_iota
    picked = jnp.sum(jnp.where(id_hot, scores[:, None, :], 0.0), -1)
    gate_weights = (picked / jnp.sum(picked, -1, keepdims=True)).astype(jnp.bfloat16)
    slots = jnp.sum(jnp.where(id_hot, placement[None, None, :], 0), -1)
    slot_hot = (
        (slots[:, :, None] == expert_iota).reshape(tok_rows * top_count, experts).astype(jnp.int32)
    )
    running = jnp.cumsum(slot_hot, 0) - 1
    position = jnp.sum(running * slot_hot, -1)
    column = slots.reshape(-1) * capacity + position
    column_iota = jnp.arange(experts * capacity, dtype=jnp.int32)
    place_hot = (column[:, None] == column_iota).reshape(tok_rows, top_count, experts * capacity)
    dispatch = jnp.any(place_hot, 1).astype(jnp.bfloat16)
    combine = jnp.sum(
        jnp.where(place_hot, gate_weights[:, :, None].astype(jnp.float32), 0.0), 1
    ).astype(jnp.bfloat16)
    flat_rows = lax.dot_general(
        dispatch, normed, (((0,), (0,)), ((), ())), preferred_element_type=jnp.float32
    ).astype(jnp.bfloat16)
    node_count = lax.axis_size("node")
    local_count = lax.axis_size("local")
    peer_count = node_count * local_count
    outgoing = flat_rows.reshape(peer_count, capacity // 2, model_width)
    piece = lax.all_to_all(outgoing, ("node", "local"), split_axis=0, concat_axis=0, tiled=True)
    partner = partner_2(piece, "local", 0)
    joined = jnp.concatenate([piece, partner], 1)
    result = feed_forward(joined.reshape(-1, model_width), w_gate, w_up, w_down).astype(
        jnp.bfloat16
    )
    result = result.reshape(joined.shape)
    own_part = result[:, : piece.shape[1]]
    their_part = result[:, piece.shape[1] :]
    back_part = partner_2(their_part, "local", 0)
    answers = (own_part.astype(jnp.float32) + back_part.astype(jnp.float32)).astype(jnp.bfloat16)
    returned = lax.all_to_all(answers, ("node", "local"), split_axis=0, concat_axis=0, tiled=True)
    expert_out = returned.reshape(experts * capacity, model_width)
    routed = jnp.dot(combine, expert_out, preferred_element_type=jnp.float32)
    return (shared + routed).astype(jnp.bfloat16)


MESH = pl.DeviceIdType.MESH


class Place:
    def __init__(self, depth):
        node, local = lax.axis_index("node"), lax.axis_index("local")
        self.depth = depth
        self.z, self.y = node // 2, node % 2
        self.x, self.c = local // 2, local % 2

    def device(self, z, y, x, c):
        return (z * 2 + y, x * 2 + c)

    def block(self, z, y, x, c):
        return ((z * 2 + y) * 2 + x) * 2 + c

    def spot(self, p):
        x = 1 - self.x if p & 1 else self.x
        y = 1 - self.y if p & 2 else self.y
        return y, x

    def greet(self):
        barrier = pltpu.get_barrier_semaphore()
        z, y, x, c = self.z, self.y, self.x, self.c

        def hello(z, y, x, c):
            pl.semaphore_signal(
                barrier, inc=1, device_id=self.device(z, y, x, c), device_id_type=MESH
            )

        hello(z, y, x, 1 - c)
        hello(z, y, 1 - x, c)
        hello(z, 1 - y, x, c)
        pl.when(z > 0)(lambda: hello(z - 1, y, x, c))
        pl.when(z < self.depth - 1)(lambda: hello(z + 1, y, x, c))
        below = (z + self.depth - 1) // self.depth
        above = (2 * self.depth - 2 - z) // self.depth
        pl.semaphore_wait(barrier, 3 + below + above)

    def at_distance(self, far, visit):
        for off in (0,) if far == 0 else (-far, far):
            other = self.z + off
            ok = other >= 0 if off <= 0 else other < self.depth
            pl.when(ok)(lambda off=off, other=other: visit(off, other))


def remote(src, dst, send, recv, device):
    return pltpu.make_async_remote_copy(
        src_ref=src, dst_ref=dst, send_sem=send, recv_sem=recv, device_id=device, device_id_type=MESH
    )


def gather_kernel(
    depth, rows, own, out, home_sem, zsend, zrecv, psend, precv, fsend, frecv, csend, crecv
):
    at = Place(depth)
    z, y, x, c = at.z, at.y, at.x, at.c
    half = rows // 2
    at.greet()
    xdev, ydev = at.device(z, y, 1 - x, c), at.device(z, 1 - y, x, c)
    partner = at.device(z, y, x, 1 - c)

    def whole(p, zz):
        yy, xx = at.spot(p)
        return out.at[at.block(zz, yy, xx, c)]

    def part(p, zz, h):
        return whole(p, zz).at[pl.ds(h * half, half)]

    def zcopy(zz, up):
        src = out.at[at.block(zz, y, x, c)]
        way = 1 if up else 0
        to = at.device(z + 1 if up else z - 1, y, x, c)
        return remote(src, src, zsend.at[zz, way], zrecv.at[zz], to)

    def plane(p, zz, h):
        return remote(
            part(0, zz, h), part(0, zz, h), psend.at[p - 1, zz, h], precv.at[p - 1, zz, h],
            xdev if p == 1 else ydev,
        )

    def relay(p, zz):
        h = p - 1
        return remote(
            part(p, zz, h), part(p, zz, h), fsend.at[h, zz], frecv.at[h, zz],
            ydev if p == 1 else xdev,
        )

    def cross(p, zz):
        return remote(whole(p, zz), whole(p, zz), csend.at[p, zz], crecv.at[p, zz], partner)

    def first(off, zz):
        if off == 0:
            home = pltpu.make_async_copy(own, whole(0, zz), home_sem)
            home.start()
            home.wait()
            pl.when(z > 0)(lambda: zcopy(zz, False).start())
            pl.when(z < depth - 1)(lambda: zcopy(zz, True).start())
        else:
            zcopy(zz, True).wait_recv()
            if off < 0:
                pl.when(z < depth - 1)(lambda: zcopy(zz, True).start())
            else:
                pl.when(z > 0)(lambda: zcopy(zz, False).start())
        plane(1, zz, 0).start()
        plane(2, zz, 1).start()
        plane(1, zz, 1).start()
        plane(2, zz, 0).start()
        cross(0, zz).start()

    def second(off, zz):
        plane(1, zz, 0).wait_recv()
        relay(1, zz).start()
        plane(2, zz, 1).wait_recv()
        relay(2, zz).start()

    def third(off, zz):
        plane(1, zz, 1).wait_recv()
        cross(1, zz).start()
        plane(2, zz, 0).wait_recv()
        cross(2, zz).start()
        relay(1, zz).wait_recv()
        relay(2, zz).wait_recv()
        cross(3, zz).start()

    def finish(off, zz):
        if off <= 0:
            pl.when(z < depth - 1)(lambda: zcopy(zz, True).wait_send())
        if off >= 0:
            pl.when(z > 0)(lambda: zcopy(zz, False).wait_send())
        for p in (1, 2):
            plane(p, zz, 0).wait_send()
            plane(p, zz, 1).wait_send()
            relay(p, zz).wait_send()
        for p in range(4):
            cross(p, zz).wait_send()
            cross(p, zz).wait_recv()

    work = []
    for far in range(depth):
        work += [(2 * far, 0, first, far), (2 * far + 1, 1, second, far), (2 * far + 4, 2, third, far)]
    for _, _, visit, far in sorted(work, key=lambda w: w[:2]):
        at.at_distance(far, visit)
    for far in range(depth):
        at.at_distance(far, finish)


def gather_rows(own, depth, peers):
    rows, width = own.shape
    sem = pltpu.SemaphoreType.DMA
    return pl.pallas_call(
        lambda *refs: gather_kernel(depth, rows, *refs),
        out_shape=jax.ShapeDtypeStruct((peers, rows, width), own.dtype),
        in_specs=[pl.BlockSpec(memory_space=pltpu.VMEM)],
        out_specs=pl.BlockSpec(memory_space=pl.ANY),
        scratch_shapes=[
            sem(()), sem((depth, 2)), sem((depth,)), sem((2, depth, 2)), sem((2, depth, 2)),
            sem((2, depth)), sem((2, depth)), sem((4, depth)), sem((4, depth)),
        ],
        compiler_params=pltpu.CompilerParams(collective_id=0, has_side_effects=True),
        name="gather_rows",
    )(own)


def scatter_kernel(
    depth, rows, sums, out, mine, theirs, turned, plane_in, z_in,
    load_sem, csend, crecv, fsend, frecv, psend, precv, zsend, zrecv,
):
    at = Place(depth)
    z, y, x, c = at.z, at.y, at.x, at.c
    half = rows // 2
    step = 16
    xdev, ydev = at.device(z, y, 1 - x, c), at.device(z, 1 - y, x, c)
    partner = at.device(z, y, x, 1 - c)

    def load(p, zz):
        yy, xx = at.spot(p)
        return pltpu.make_async_copy(
            sums.at[at.block(zz, yy, xx, c)], mine.at[p, zz], load_sem.at[p, zz]
        )

    def cross(p, zz):
        yy, xx = at.spot(p)
        return remote(
            sums.at[at.block(zz, yy, xx, 1 - c)], theirs.at[p, zz],
            csend.at[p, zz], crecv.at[p, zz], partner,
        )

    def turn(p, zz):
        h = p - 1
        return remote(
            mine.at[3, zz, pl.ds(h * half, half)], turned.at[h, zz],
            fsend.at[h, zz], frecv.at[h, zz], xdev if p == 1 else ydev,
        )

    def plane(p, zz, h):
        piece = pl.ds(h * half, half)
        return remote(
            mine.at[p, zz, piece], plane_in.at[p - 1, zz, piece],
            psend.at[p - 1, zz, h], precv.at[p - 1, zz, h], xdev if p == 1 else ydev,
        )

    def zcopy(zz, up):
        way = 1 if up else 0
        to = at.device(z + 1 if up else z - 1, y, x, c)
        return remote(mine.at[0, zz], z_in.at[way, zz], zsend.at[zz, way], zrecv.at[zz, way], to)

    def add(into, terms, count):
        def one(i, carry):
            piece = pl.ds(pl.multiple_of(i * step, step), step)
            total = into[piece].astype(jnp.float32)
            for term in terms:
                total = total + term[piece].astype(jnp.float32)
            into[piece] = total.astype(into.dtype)
            return carry

        lax.fori_loop(0, count // step, one, 0)

    def begin(off, zz):
        for p in (3, 1, 2, 0):
            load(p, zz).start()

    def begin_cross(off, zz):
        for p in (3, 1, 2, 0):
            cross(p, zz).start()

    def first(off, zz):
        for p in (3, 1, 2, 0):
            load(p, zz).wait()
            cross(p, zz).wait_recv()
            add(mine.at[p, zz], [theirs.at[p, zz]], rows)
            if p == 3:
                turn(1, zz).start()
                turn(2, zz).start()
            if p == 1:
                plane(1, zz, 0).start()
            if p == 2:
                plane(2, zz, 1).start()

    def second(off, zz):
        turn(1, zz).wait_recv()
        add(mine.at[2, zz, pl.ds(0, half)], [turned.at[0, zz]], half)
        plane(2, zz, 0).start()
        turn(2, zz).wait_recv()
        add(mine.at[1, zz, pl.ds(half, half)], [turned.at[1, zz]], half)
        plane(1, zz, 1).start()

    def third(off, zz):
        for p in (1, 2):
            for h in (0, 1):
                plane(p, zz, h).wait_recv()
        add(mine.at[0, zz], [plane_in.at[0, zz], plane_in.at[1, zz]], rows)
        if off <= 0:

            @pl.when(z < depth - 1)
            def _():
                zcopy(zz, False).wait_recv()
                add(mine.at[0, zz], [z_in.at[0, zz]], rows)

        if off >= 0:

            @pl.when(z > 0)
            def _():
                zcopy(zz, True).wait_recv()
                add(mine.at[0, zz], [z_in.at[1, zz]], rows)

        if off < 0:
            zcopy(zz, False).start()
        if off > 0:
            zcopy(zz, True).start()
        if off == 0:

            def put(i, carry):
                piece = pl.ds(pl.multiple_of(i * step, step), step)
                out[piece] = mine[0, zz, piece]
                return carry

            lax.fori_loop(0, rows // step, put, 0)

    def finish(off, zz):
        for p in range(4):
            cross(p, zz).wait_send()
        for p in (1, 2):
            turn(p, zz).wait_send()
            plane(p, zz, 0).wait_send()
            plane(p, zz, 1).wait_send()
        if off < 0:
            zcopy(zz, False).wait_send()
        if off > 0:
            zcopy(zz, True).wait_send()

    for far in reversed(range(depth)):
        at.at_distance(far, begin)
    at.greet()
    for far in reversed(range(depth)):
        at.at_distance(far, begin_cross)
    work = []
    for far in range(depth):
        turn_no = 2 * (depth - 1 - far)
        work += [(turn_no, 0, first, far), (turn_no + 3, 1, second, far), (turn_no + 5, 2, third, far)]
    for _, _, visit, far in sorted(work, key=lambda w: w[:2]):
        at.at_distance(far, visit)
    for far in range(depth):
        at.at_distance(far, finish)


def scatter_sums(sums, depth):
    _, rows, width = sums.shape
    sem = pltpu.SemaphoreType.DMA
    vmem = lambda *lead: pltpu.VMEM(lead + (width,), sums.dtype)
    return pl.pallas_call(
        lambda *refs: scatter_kernel(depth, rows, *refs),
        out_shape=jax.ShapeDtypeStruct((rows, width), sums.dtype),
        in_specs=[pl.BlockSpec(memory_space=pl.ANY)],
        out_specs=pl.BlockSpec(memory_space=pltpu.VMEM),
        scratch_shapes=[
            vmem(4, depth, rows), vmem(4, depth, rows), vmem(2, depth, rows // 2),
            vmem(2, depth, rows), vmem(2, depth, rows),
            sem((4, depth)), sem((4, depth)), sem((4, depth)), sem((2, depth)), sem((2, depth)),
            sem((2, depth, 2)), sem((2, depth, 2)), sem((depth, 2)), sem((depth, 2)),
        ],
        compiler_params=pltpu.CompilerParams(
            collective_id=1, has_side_effects=True, vmem_limit_bytes=48 * 1024 * 1024
        ),
        name="scatter_sums",
    )(sums)


def gathered_body(
    tokens, norm_gain, router_weight, placement, expert_ids,
    w_gate, w_up, w_down, shared_gate, shared_up, shared_down,
):
    node_count, local_count = lax.axis_size("node"), lax.axis_size("local")
    peers = node_count * local_count
    node, local = lax.axis_index("node"), lax.axis_index("local")
    floats = tokens.astype(jnp.float32)
    normed = (
        floats * lax.rsqrt(jnp.mean(floats * floats, -1, keepdims=True) + 1e-06) * norm_gain
    ).astype(jnp.bfloat16)
    rows, width = normed.shape
    experts, top_count = placement.shape[0], expert_ids.shape[1]
    capacity = min(rows, 3 * rows * top_count // (2 * experts))
    scores = jax.nn.sigmoid(jnp.dot(normed, router_weight, preferred_element_type=jnp.float32))
    id_hot = expert_ids[:, :, None] == jnp.arange(experts, dtype=jnp.int32)
    named = jnp.any(id_hot, 1)
    chosen = jnp.where(named, scores, 0.0)
    gates = chosen / jnp.sum(chosen, -1, keepdims=True)
    lanes = -(-experts // 128) * 128
    slot_hot = placement[:, None] == jnp.arange(lanes, dtype=jnp.int32)
    by_slot = jnp.sum(jnp.where(slot_hot[None], gates[:, :, None], 0.0), 1).astype(jnp.bfloat16)
    block = gather_rows(jnp.concatenate([normed, by_slot], 1), node_count // 2, peers)
    all_rows = block[:, :, :width]
    slot = (node * local_count + local) // 2
    mine = jnp.arange(lanes, dtype=jnp.int32) == slot
    weight = jnp.sum(jnp.where(mine, block[:, :, width:].astype(jnp.float32), 0.0), -1)
    taken = weight > 0
    spot = jnp.cumsum(taken.astype(jnp.int32), 1) - 1
    row_hot = (spot[:, None, :] == jnp.arange(capacity, dtype=jnp.int32)[:, None]) & taken[:, None, :]
    pick = row_hot.astype(jnp.bfloat16)
    back = jnp.where(row_hot, weight[:, None, :], 0.0).astype(jnp.bfloat16)
    packed = lax.dot_general(
        pick, all_rows, (((2,), (1,)), ((0,), (0,))), preferred_element_type=jnp.float32
    ).astype(jnp.bfloat16)
    result = feed_forward(packed.reshape(peers * capacity, width), w_gate, w_up, w_down)
    result = result.astype(jnp.bfloat16).reshape(peers, capacity, width)
    sums = lax.dot_general(
        back, result, (((1,), (1,)), ((0,), (0,))), preferred_element_type=jnp.float32
    ).astype(jnp.bfloat16)
    near = lax.dynamic_slice_in_dim(all_rows, node * local_count, local_count, 0)
    shared = feed_forward(near.reshape(-1, width), shared_gate, shared_up, shared_down)
    old = lax.dynamic_slice_in_dim(sums, node * local_count, local_count, 0)
    new = (old.astype(jnp.float32) + shared.reshape(old.shape)).astype(jnp.bfloat16)
    sums = lax.dynamic_update_slice_in_dim(sums, new, node * local_count, 0)
    return scatter_sums(sums, node_count // 2)


def solution(mesh):
    in_specs = (
        P(("node", "local"), None),
        P(),
        P(),
        P(),
        P(("node", "local"), None),
        P(None, ("node", "local")),
        P(None, ("node", "local")),
        P(("node", "local"), None),
        P(None, "local"),
        P(None, "local"),
        P("local", None),
    )
    out_specs = P(("node", "local"), None)
    plane_of_four = mesh.shape["local"] == 4 and mesh.shape["node"] % 2 == 0

    def chosen(*args):
        pairs = mesh.size == 2 * args[3].shape[0]
        small = args[0].size * args[0].dtype.itemsize <= 24 * 2**20
        plan = gathered_body if plane_of_four and pairs and small else body
        return jax.shard_map(
            plan, mesh=mesh, in_specs=in_specs, out_specs=out_specs, check_vma=False
        )(*args)

    return chosen
```
